32 devices in a mesh: groups: 2 (over y), dom: 4 (over z), ens: 4 (over x, core).
Axes of the slice: x: 2, y: 2, z: 4, core: 2. Of those that a mesh axis runs over, the one named last changes fastest.
Arguments:
- state: float32 [16, 256, 512], P('ens', ('groups', 'dom')), parts along dimension 1, may hold values from -8 to 8, as said below
- coords: float32 [3, 2048], P(None, ('groups', 'dom')), parts along dimension 1, may hold values from -1 to 1
- owner_local: int32 [2048], P(('groups', 'dom')), parts along dimension 0, may hold values from 0 to 31
- counts: int32 [8, 4], P(('groups', 'dom')), parts along dimension 0, may hold values from 32 to 64, as said below
- obs_value: float32 [2048], P(('groups', 'dom')), parts along dimension 0, may hold values from 0.5 to 3.5
- obs_weight: float32 [2048], P(('groups', 'dom')), parts along dimension 0, as said below
Outputs:
- analysis: float32 [16, 256, 512], P('ens', ('groups', 'dom')), parts along dimension 1
The draws below stay inside these ranges and needn't reach their ends.
There are 2 independent parts, one for each index of `groups`. The reference program is written for one: setup_inputs(seed, part) draws one part's arguments, and reference() takes and returns one part's arrays. A program takes and returns all parts, laid end to end along the dimension named above; each array names one. Nothing has to cross between parts.
Inputs may be any that keep to these rules, and one draw needn't show every extreme that they name: `state`: each member is an independent field plus an offset of its own. The sensors of one block are stored in order of owner block: the first counts[d, 0] slots belong to owner block 0, the next counts[d, 1] to block 1, and so on; slots after the last of them are unused. For one owner block, chosen by the draw, every row holds exactly 64. `obs_weight`: Positive.
All inputs are finite; a program needn't handle non-finite values.
Results may differ from the reference program's by a relative error of at most 0.00028.
Values sent between devices are 32-bit elements; how exact they have to be, the bound alone decides.
A program may use at most 64 MiB of HBM per device.

```python
import math
import jax
import jax.numpy as jnp
from jax import lax

NODES = 512
MEMBERS = 16
ELEM_DEV = 32
ELEMENTS = 128
CAP = 64
OBS_DEV = 256
OBS_TOTAL = 1024
NS_ITERS = 8
N_DOM = 4


def draw_state(key, part):
    noise_key, offset_key = jax.random.split(jax.random.fold_in(key, 11))
    noise = jnp.clip(jax.random.normal(noise_key, (MEMBERS, ELEMENTS, NODES), jnp.float32), -5.0, 5.0)
    offset = jnp.clip(jax.random.normal(offset_key, (MEMBERS, 1, 1), jnp.float32), -3.0, 3.0)
    return noise + offset


def draw_counts(key, part):
    hot_key, count_key = jax.random.split(jax.random.fold_in(key, 23))
    hot_owner = jax.random.randint(hot_key, (), 0, N_DOM)
    base_counts = jax.random.randint(count_key, (N_DOM, N_DOM), CAP // 2, CAP + 1)
    column = jnp.arange(N_DOM, dtype=jnp.int32)
    return jnp.where(column[None, :] == hot_owner, CAP, base_counts).astype(jnp.int32)


def draw_obs_weight(key, part):
    base_key = jax.random.fold_in(key, 37)
    block_number = jnp.arange(OBS_TOTAL, dtype=jnp.int32) // OBS_DEV
    rising = 1.0 + 2.0 * block_number.astype(jnp.float32) / max(N_DOM - 1, 1)
    scale_value = 50.0 / (N_DOM * (3 * N_DOM + 1) * CAP)
    base_weight = jnp.exp(jax.random.uniform(base_key, (OBS_TOTAL,), jnp.float32, 0.0, math.log(10.0)))
    return (base_weight * rising * scale_value).astype(jnp.float32)


def with_ends(array, key, smallest, top_value):
    longest = array.shape.index(max(array.shape))
    spots = []
    for shift in (0, 1):
        where = [jax.random.randint(jax.random.fold_in(key, axis), (), 0, length) for axis, length in enumerate(array.shape)]
        where[longest] = (where[longest] + shift) % array.shape[longest]
        spots.append(tuple(where))
    return array.at[spots[0]].set(smallest).at[spots[1]].set(top_value)


def shard_levels(own_key, dims, cuts, low, high):
    factor_of, own = 1.0, jax.random.fold_in(own_key, 6)
    for dim, parts in cuts:
        draws = jnp.exp(jax.random.uniform(jax.random.fold_in(own, dim), (parts,), jnp.float32, low / len(cuts), high / len(cuts)))
        factor_of = factor_of * jnp.repeat(draws, dims[dim] // parts).reshape([-1 if axis == dim else 1 for axis in range(len(dims))])
    return factor_of


def setup_inputs(seed: int = 0, part: int = 0) -> dict:
    streams_of = jax.random.split(jax.random.key(seed), 7)
    part_keys = jax.random.split(jax.random.fold_in(streams_of[6], part), 7)
    return {
        "state": draw_state(jax.random.fold_in(jax.random.fold_in(streams_of[6], part), 71), part),
        "coords": jnp.clip(jax.random.uniform(part_keys[1], (3, OBS_TOTAL), jnp.float32, -1.0, 1.0) * shard_levels(part_keys[1], (3, OBS_TOTAL), ((1, 4),), -0.4, 0.0), -1.0, 1.0),
        "owner_local": with_ends(jax.random.randint(part_keys[2], (OBS_TOTAL,), 0, ELEM_DEV), jax.random.fold_in(part_keys[2], 1), 0, ELEM_DEV - 1).astype(jnp.int32),
        "counts": draw_counts(jax.random.fold_in(jax.random.fold_in(streams_of[6], part), 71), part),
        "obs_value": jnp.clip(0.5 + 3.0 * jax.random.uniform(part_keys[4], (OBS_TOTAL,), jnp.float32) ** shard_levels(part_keys[4], (OBS_TOTAL,), ((0, 4),), -0.2, 0.2), 0.5, 3.5),
        "obs_weight": draw_obs_weight(jax.random.fold_in(jax.random.fold_in(streams_of[6], part), 71), part),
    }


GLL_POINTS = (-1.0, -0.8717401485096066, -0.5917001814331423, -0.2092992179024789, 0.2092992179024789, 0.5917001814331423, 0.8717401485096066, 1.0)
INFLATION = 1.1

def lagrange(position):
    basis_rows = []
    for node_index in range(8):
        product = jnp.ones_like(position)
        for other_node in range(8):
            if other_node != node_index:
                product = product * (position - GLL_POINTS[other_node]) / (GLL_POINTS[node_index] - GLL_POINTS[other_node])
        basis_rows.append(product)
    return jnp.stack(basis_rows, 0)

def node_weights(sensor_coords):
    along_r = lagrange(sensor_coords[0]).T
    along_s = lagrange(sensor_coords[1]).T
    along_t = lagrange(sensor_coords[2]).T
    node_table = along_t[:, :, None, None] * along_s[:, None, :, None] * along_r[:, None, None, :]
    return node_table.reshape(sensor_coords.shape[1], 512)

def analysis_weights(cross_terms, project):
    highest = lax.Precision.HIGHEST
    members = cross_terms.shape[0]
    identity = jnp.eye(members, dtype=jnp.float32)
    system = cross_terms + (members - 1) / INFLATION * identity
    trace_value = jnp.trace(system)
    iterate = system / trace_value
    inverse_root = identity
    for sweep in range(NS_ITERS):
        middle = 0.5 * (3.0 * identity - jnp.dot(inverse_root, iterate, precision=highest))
        iterate = jnp.dot(iterate, middle, precision=highest)
        inverse_root = jnp.dot(middle, inverse_root, precision=highest)
    mean_weights = jnp.dot(inverse_root, jnp.dot(inverse_root, project, precision=highest), precision=highest) / trace_value
    transform = inverse_root * jnp.sqrt((members - 1) / trace_value) + mean_weights[:, None]
    return transform - lax.optimization_barrier(jnp.mean(transform, axis=0, keepdims=True)) + 1.0 / members

def reference(state, coords, owner_local, counts, obs_value, obs_weight):
    highest = lax.Precision.HIGHEST
    members = state.shape[0]
    segment_ends = jnp.cumsum(counts, axis=1)
    slot_index = jnp.arange(OBS_DEV, dtype=jnp.int32)
    destination = lax.optimization_barrier(jnp.sum((slot_index[None, :, None] >= segment_ends[:, None, :]).astype(jnp.int32), axis=2))
    in_use = destination < N_DOM
    element = jnp.minimum(destination, N_DOM - 1) * ELEM_DEV + owner_local.reshape(N_DOM, OBS_DEV)
    used_weight = jnp.where(in_use.reshape(-1), obs_weight, jnp.zeros_like(obs_weight))

    def interpolate(inputs):
        block_coords, block_element = inputs
        node_table = node_weights(block_coords)
        element_rows = jnp.take(state, block_element, axis=1)
        return jnp.einsum('sn,ksn->ks', node_table, element_rows, precision=highest)
    block_coords = coords.reshape(3, N_DOM, OBS_DEV).transpose(1, 0, 2)
    model_value = lax.map(interpolate, (block_coords, element))
    model_value = model_value.transpose(1, 0, 2).reshape(members, N_DOM * OBS_DEV)
    mean_value = lax.optimization_barrier(jnp.mean(model_value, axis=0))
    anomaly = model_value - mean_value[None, :]
    weighted = anomaly * used_weight[None, :]
    cross_terms = jnp.dot(weighted, anomaly.T, precision=highest)
    project = jnp.dot(weighted, obs_value - mean_value, precision=highest)
    mixing = analysis_weights(cross_terms, project)
    flat_state = state.reshape(members, -1)
    return jnp.dot(mixing.T, flat_state, precision=highest).reshape(state.shape)
```

```python
import functools

import jax
import jax.numpy as jnp
from jax import lax
from jax.experimental import pallas as pl
from jax.experimental.pallas import tpu as pltpu
from jax.sharding import PartitionSpec as P

NS_ITERS = 8
GLL_POINTS = (
    -1.0,
    -0.8717401485096066,
    -0.5917001814331423,
    -0.2092992179024789,
    0.2092992179024789,
    0.5917001814331423,
    0.8717401485096066,
    1.0,
)
INFLATION = 1.1
LANES = 128
FOUR = 4
MESH = pl.DeviceIdType.MESH
F32 = jnp.float32
BF16 = jnp.bfloat16


def each(count, body):
    if count <= 8:
        for index in range(count):
            body(index)
    else:
        lax.fori_loop(0, count, lambda index, _: (body(index), 0)[1], 0)


def halves(value):
    high = value.astype(BF16)
    return high, (value - high.astype(F32)).astype(BF16)


def dot(a, b, contract=((1,), (0,))):
    return lax.dot_general(
        a,
        b,
        (contract, ((), ())),
        precision=lax.Precision.HIGHEST,
        preferred_element_type=F32,
    )


def lagrange(position):
    shape = (8, position.shape[1])
    row = lax.broadcasted_iota(jnp.int32, shape, 0)
    x = jnp.broadcast_to(position, shape)
    product = jnp.zeros(shape, F32)
    for a in range(8):
        scale = 1.0
        for b in range(8):
            if b != a:
                scale /= GLL_POINTS[a] - GLL_POINTS[b]
        product = jnp.where(row == a, scale, product)
    for b in range(8):
        product = product * jnp.where(row == b, 1.0, x - GLL_POINTS[b])
    return product


def kernel(
    n_dom,
    n_ens,
    counts_hbm,
    coords_hbm,
    owner_hbm,
    value_hbm,
    weight_hbm,
    state_ref,
    out_ref,
    counts_ref,
    coords_ref,
    owner_ref,
    value_ref,
    weight_ref,
    packed,
    sensors,
    gathered,
    state_high,
    state_low,
    values,
    partial,
    mix_rows,
    small_sem,
    load_sem,
    sensor_send,
    sensor_recv,
    value_send,
    value_recv,
    part_send,
    part_recv,
    near_sem,
    far_send,
    far_recv,
    pass_send,
    pass_recv,
):
    d = lax.axis_index("dom")
    e = lax.axis_index("ens")
    local_members, local_elements, nodes = state_ref.shape
    members = local_members * n_ens
    slots = coords_hbm.shape[1]
    cap = slots // n_dom
    near = e + 1 - 2 * lax.rem(e, 2)
    far = lax.rem(e + 2, n_ens)

    barrier = pltpu.get_barrier_semaphore()
    for axis, me, count in (("dom", d, n_dom), ("ens", e, n_ens)):
        for off in range(1, count):
            pl.semaphore_signal(
                barrier, inc=1, device_id={axis: lax.rem(me + off, count)}, device_id_type=MESH
            )
    small = [
        pltpu.make_async_copy(source, target, small_sem.at[index])
        for index, (source, target) in enumerate(
            (
                (counts_hbm, counts_ref),
                (coords_hbm, coords_ref),
                (owner_hbm, owner_ref),
                (value_hbm, value_ref),
                (weight_hbm, weight_ref),
            )
        )
    ]
    for copy in small:
        copy.start()
    load = pltpu.make_async_copy(state_ref, gathered.at[e], load_sem)
    load.start()
    for copy in small:
        copy.wait()

    zero = jnp.zeros((2, slots), F32)
    feature = jnp.concatenate(
        [
            coords_ref[...],
            owner_ref[...].astype(F32),
            value_ref[...],
            weight_ref[...],
            zero,
        ],
        axis=0,
    )
    slot = lax.broadcasted_iota(jnp.int32, (slots, LANES), 0)
    lane = lax.broadcasted_iota(jnp.int32, (slots, LANES), 1) - lax.rem(d, 2) * cap

    def pack(q, start):
        count = counts_ref[0, q]
        wanted = jnp.where((lane >= 0) & (lane < count), lane + start, -1)
        packed[q] = dot(feature, (slot == wanted).astype(F32))
        return start + count

    if n_dom <= 8:
        start = jnp.int32(0)
        for q in range(n_dom):
            start = pack(q, start)
    else:
        lax.fori_loop(0, n_dom, pack, jnp.int32(0))
    sensors[d] = packed[d]

    load.wait()
    high, low = halves(gathered[e].reshape(local_members * local_elements, nodes))
    state_high[...] = high
    state_low[...] = low

    pl.semaphore_wait(barrier, n_dom - 1 + n_ens - 1)

    def sensor_copy(off):
        to = lax.rem(d + off, n_dom)
        return pltpu.make_async_remote_copy(
            src_ref=packed.at[to],
            dst_ref=sensors.at[d],
            send_sem=sensor_send.at[off],
            recv_sem=sensor_recv.at[off],
            device_id={"dom": to},
            device_id_type=MESH,
        )

    def far_copy(m):
        return pltpu.make_async_remote_copy(
            src_ref=gathered.at[e, m],
            dst_ref=gathered.at[e, m],
            send_sem=far_send.at[m],
            recv_sem=far_recv.at[m],
            device_id={"ens": far},
            device_id_type=MESH,
        )

    def pass_copy(m):
        return pltpu.make_async_remote_copy(
            src_ref=gathered.at[far, m],
            dst_ref=gathered.at[far, m],
            send_sem=pass_send.at[m],
            recv_sem=pass_recv.at[m],
            device_id={"ens": near},
            device_id_type=MESH,
        )

    near_copy = pltpu.make_async_remote_copy(
        src_ref=gathered.at[e],
        dst_ref=gathered.at[e],
        send_sem=near_sem.at[0],
        recv_sem=near_sem.at[1],
        device_id={"ens": near},
        device_id_type=MESH,
    )

    each(n_dom - 1, lambda i: sensor_copy(i + 1).start())
    early = local_members // 2
    for m in range(early):
        far_copy(m).start()
    near_copy.start()
    each(n_dom - 1, lambda i: sensor_copy(i + 1).wait_recv())

    width = FOUR * cap
    value_row = lax.broadcasted_iota(jnp.int32, (8, width), 0) - lax.rem(e * local_members, 8)
    element = lax.broadcasted_iota(jnp.int32, (local_elements, width), 0).astype(F32)

    def columns(c):
        return jnp.concatenate(
            [
                sensors[c * FOUR + 2 * pair] + sensors[c * FOUR + 2 * pair + 1]
                for pair in range(FOUR // 2)
            ],
            axis=1,
        )

    def interpolate(c):
        data = columns(c)
        along_r = lagrange(data[0:1])
        along_s = lagrange(data[1:2])
        along_t = lagrange(data[2:3])
        table = []
        for t in range(8):
            for s in range(8):
                table.append(along_r * (along_s[s : s + 1] * along_t[t : t + 1]))
        table_high, table_low = halves(jnp.concatenate(table, axis=0))
        product = functools.partial(jnp.dot, preferred_element_type=F32)
        found = product(state_high[...], table_high) + (
            product(state_high[...], table_low) + product(state_low[...], table_high)
        )
        mine = element == data[3:4]
        block = jnp.zeros((8, width), F32)
        for m in range(local_members):
            rows = found[m * local_elements : (m + 1) * local_elements]
            chosen = jnp.sum(jnp.where(mine, rows, 0.0), axis=0, keepdims=True)
            block = jnp.where(value_row == m, chosen, block)
        values[e, c] = block

    chunks = n_dom // FOUR
    each(chunks, interpolate)

    def value_copy(off):
        return pltpu.make_async_remote_copy(
            src_ref=values.at[e],
            dst_ref=values.at[e],
            send_sem=value_send.at[off],
            recv_sem=value_recv.at[off],
            device_id={"ens": lax.rem(e + off, n_ens)},
            device_id_type=MESH,
        )

    for off in range(1, n_ens):
        value_copy(off).start()
    for m in range(early, local_members):
        far_copy(m).start()
    for m in range(early):
        far_copy(m).wait_recv()
        pass_copy(m).start()
    for off in range(1, n_ens):
        value_copy(off).wait_recv()

    share = 8 // local_members

    def products(c, sums):
        data = columns(c)
        rows = []
        for first in range(0, n_ens, share):
            tile = values[first, c]
            for other in range(1, share):
                tile = tile + values[first + other, c]
            rows.append(tile)
        model = jnp.concatenate(rows, axis=0)
        mean_value = jnp.mean(model, axis=0, keepdims=True)
        anomaly = model - mean_value
        weighted = anomaly * data[5:6]
        innovation = jnp.broadcast_to(data[4:5] - mean_value, anomaly.shape)
        square = jnp.sum(weighted * anomaly, keepdims=True)
        both = jnp.concatenate([anomaly, innovation], axis=0)
        return sums[0] + dot(weighted, both, ((1,), (1,))), sums[1] + square

    none = (jnp.zeros((members, 2 * members), F32), jnp.zeros((1, 1), F32))
    if chunks == 1:
        sums = products(0, none)
    else:
        sums = lax.fori_loop(0, chunks, products, none)
    partial[d, 0:members, 0 : 2 * members] = sums[0]
    partial[d, members:, :] = jnp.broadcast_to(sums[1], (8, LANES))

    def part_copy(off):
        return pltpu.make_async_remote_copy(
            src_ref=partial.at[d],
            dst_ref=partial.at[d],
            send_sem=part_send.at[off],
            recv_sem=part_recv.at[off],
            device_id={"dom": lax.rem(d + off, n_dom)},
            device_id_type=MESH,
        )

    each(n_dom - 1, lambda i: part_copy(i + 1).start())
    for m in range(early, local_members):
        far_copy(m).wait_recv()
        pass_copy(m).start()
    each(n_dom - 1, lambda i: part_copy(i + 1).wait_recv())

    if n_dom <= 8:
        total = partial[0]
        for q in range(1, n_dom):
            total = total + partial[q]
    else:
        total = lax.fori_loop(
            0, n_dom, lambda q, sums: sums + partial[q], jnp.zeros((members + 8, LANES), F32)
        )
    shape = (members, LANES)
    row = lax.broadcasted_iota(jnp.int32, shape, 0)
    lane = lax.broadcasted_iota(jnp.int32, shape, 1)
    diagonal = (row == lane).astype(F32)
    ridge = (members - 1) / INFLATION
    trace_value = jnp.concatenate(
        [total[members : members + 8]] * (members // 8), axis=0
    ) + members * ridge
    total = total[:members]
    system = jnp.where(lane < members, total + ridge * diagonal, total)
    squared = jnp.where(lane < members, system / trace_value, total)
    single = (row + members == lane + e * local_members).astype(F32)
    for sweep in range(NS_ITERS):
        middle = 1.5 * diagonal - 0.5 * squared
        columns_of = [
            jnp.broadcast_to(middle[:, k : k + 1], shape) for k in range(members)
        ]

        def times(operand):
            terms = [
                columns_of[k] * jnp.broadcast_to(operand[k : k + 1, :], shape)
                for k in range(members)
            ]
            while len(terms) > 1:
                terms = [terms[i] + terms[i + 1] for i in range(0, len(terms), 2)]
            return terms[0]

        squared = times(times(squared))
        single = times(single)
    transform = single * jnp.sqrt((members - 1) / trace_value) + squared / trace_value
    mixing = transform - jnp.mean(transform, axis=0, keepdims=True) + 1.0 / members
    for k in range(local_members):
        mix_rows[:, k * LANES : (k + 1) * LANES] = jnp.broadcast_to(
            mixing[:, members + k : members + k + 1], shape
        )

    near_copy.wait_recv()
    for m in range(local_members):
        pass_copy(m).wait_recv()

    for part in range(nodes // LANES):
        where = slice(part * LANES, (part + 1) * LANES)
        sums = [None] * local_members
        for j in range(members):
            field = gathered[j // local_members, j % local_members, :, where]
            for k in range(local_members):
                term = mix_rows[j : j + 1, k * LANES : (k + 1) * LANES] * field
                sums[k] = term if sums[k] is None else sums[k] + term
        for k in range(local_members):
            out_ref[k, :, where] = sums[k]

    each(n_dom - 1, lambda i: sensor_copy(i + 1).wait_send())
    each(n_dom - 1, lambda i: part_copy(i + 1).wait_send())
    for off in range(1, n_ens):
        value_copy(off).wait_send()
    near_copy.wait_send()
    for m in range(local_members):
        far_copy(m).wait_send()
        pass_copy(m).wait_send()


def on_device(n_dom, n_ens, state, coords, owner_local, counts, obs_value, obs_weight):
    local_members, local_elements, nodes = state.shape
    slots = coords.shape[1]
    width = FOUR * (slots // n_dom)
    members = local_members * n_ens
    rows = local_members * local_elements
    dma = pltpu.SemaphoreType.DMA
    return pl.pallas_call(
        functools.partial(kernel, n_dom, n_ens),
        out_shape=pltpu.VMEM(state.shape, F32),
        in_specs=[pl.BlockSpec(memory_space=pl.ANY)] * 6,
        out_specs=pl.BlockSpec(memory_space=pltpu.VMEM),
        scratch_shapes=[
            pltpu.SMEM((1, n_dom), jnp.int32),
            pltpu.VMEM(coords.shape, F32),
            pltpu.VMEM((1, slots), jnp.int32),
            pltpu.VMEM((1, slots), F32),
            pltpu.VMEM((1, slots), F32),
            pltpu.VMEM((n_dom, 8, LANES), F32),
            pltpu.VMEM((n_dom, 8, LANES), F32),
            pltpu.VMEM((n_ens,) + state.shape, F32),
            pltpu.VMEM((rows, nodes), BF16),
            pltpu.VMEM((rows, nodes), BF16),
            pltpu.VMEM((n_ens, n_dom // FOUR, 8, width), F32),
            pltpu.VMEM((n_dom, members + 8, LANES), F32),
            pltpu.VMEM((members, local_members * LANES), F32),
            dma((5,)),
            dma,
            dma((n_dom,)),
            dma((n_dom,)),
            dma((n_ens,)),
            dma((n_ens,)),
            dma((n_dom,)),
            dma((n_dom,)),
            dma((2,)),
            dma((local_members,)),
            dma((local_members,)),
            dma((local_members,)),
            dma((local_members,)),
        ],
        compiler_params=pltpu.CompilerParams(collective_id=0, has_side_effects=True),
        name="analysis",
    )(
        counts,
        coords,
        owner_local.reshape(1, slots),
        obs_value.reshape(1, slots),
        obs_weight.reshape(1, slots),
        state,
    )


def solution(mesh):
    return jax.shard_map(
        functools.partial(on_device, mesh.shape["dom"], mesh.shape["ens"]),
        mesh=mesh,
        in_specs=(
            P("ens", ("groups", "dom"), None),
            P(None, ("groups", "dom")),
            P(("groups", "dom")),
            P(("groups", "dom"), None),
            P(("groups", "dom")),
            P(("groups", "dom")),
        ),
        out_specs=P("ens", ("groups", "dom"), None),
        check_vma=False,
    )
```
